32 devices in a mesh: bank: 2 (over x), basis: 16 (over z, y, core).
Axes of the slice: x: 2, y: 2, z: 4, core: 2. Of those that a mesh axis runs over, the one named last changes fastest.
Arguments:
- strain: float32 [256, 4, 2, 128], P('basis'), may hold values from -6 to 6
- basis_vectors: bfloat16 [64, 256, 2, 128], P(('bank', 'basis')), parts along dimension 0, may hold values from -0.0234375 to 0.0234375
- coefficients: float32 [512, 2, 32], P(('bank', 'basis')), parts along dimension 0, may hold values from -0.75 to 0.75
- template_rows: int32 [512], P('bank'), parts along dimension 0, may hold values from 0 to 255
Outputs:
- snr_power: float32 [4, 512, 256, 256], P(None, 'bank', 'basis'), parts along dimension 1
The draws below stay inside these ranges and needn't reach their ends.
There are 2 independent parts, one for each index of `bank`. The reference program is written for one: setup_inputs(seed, part) draws one part's arguments, and reference() takes and returns one part's arrays. A program takes and returns all parts, laid end to end along the dimension named above; an argument that names none is the same for every part. Nothing has to cross between parts.
Inputs may be any that keep to these rules, and one draw needn't show every extreme that they name: template_rows[j] is the coefficient row of the j-th of the 256 rebuilt templates, the same for every sample.
All inputs are finite; a program needn't handle non-finite values.
Results may differ from the reference program's by a relative error of at most 0.0041.
Values may be sent and summed in bfloat16 or wider, within the bound.
No kernel may reach another device: no remote copies, remote signals or barrier semaphores. Data moves between devices by JAX's collectives and lax.ppermute only.
A program may use at most 192 MiB of HBM per device.

```python
import jax
import jax.numpy as jnp
from jax import lax

SIDE = 256
SAMPLES = 65536
BASIS_VECS = 32
SEG = 4
TEMPLATES = 256
BANK_ROWS = 256
N_BASIS = 16


def with_ends(entries, own_key, least, high):
    longest = entries.shape.index(max(entries.shape))
    spots = []
    for shift in (0, 1):
        where = [jax.random.randint(jax.random.fold_in(own_key, axis), (), 0, length) for axis, length in enumerate(entries.shape)]
        where[longest] = (where[longest] + shift) % entries.shape[longest]
        spots.append(tuple(where))
    return entries.at[spots[0]].set(least).at[spots[1]].set(high)


def steps_of(rng, shape, split, low, high):
    gain, own = 1.0, jax.random.fold_in(rng, 6)
    for dim, shards_of in split:
        draws = jnp.exp(jax.random.uniform(jax.random.fold_in(own, dim), (shards_of,), jnp.float32, low / len(split), high / len(split)))
        gain = gain * jnp.repeat(draws, shape[dim] // shards_of).reshape([-1 if axis == dim else 1 for axis in range(len(shape))])
    return gain


def gaussian(own_key, dims, deviation, bound, cuts=(), dtype=jnp.bfloat16):
    entries = deviation * jax.random.normal(own_key, dims, jnp.float32)
    if cuts:
        entries = entries * steps_of(own_key, dims, cuts, -0.22, 0.18)
    return jnp.clip(entries, -bound, bound).astype(dtype)


def setup_inputs(seed: int = 0, part: int = 0) -> dict:
    keys = jax.random.split(jax.random.key(seed), 5)
    own_keys = jax.random.split(jax.random.fold_in(keys[4], part), 5)
    strain = gaussian(keys[0], (SIDE, SEG, 2, SIDE // 2), 1.0, 6.0, ((0, 16),), jnp.float32)
    basis_vectors = gaussian(own_keys[1], (BASIS_VECS, SIDE, 2, SIDE // 2), (SIDE * SIDE) ** -0.5, 0.0234375, ((0, 16),))
    coefficients = gaussian(own_keys[2], (BANK_ROWS, 2, BASIS_VECS), (2 * BASIS_VECS) ** -0.5, 0.75, ((0, 16),), jnp.float32)
    template_rows = with_ends(jax.random.randint(own_keys[3], (TEMPLATES,), 0, BANK_ROWS), jax.random.fold_in(own_keys[3], 1), 0, BANK_ROWS - 1).astype(jnp.int32)
    return {"strain": strain, "basis_vectors": basis_vectors, "coefficients": coefficients, "template_rows": template_rows}


highest = lax.Precision.HIGHEST


def rounded(values):
    return lax.optimization_barrier(values.astype(jnp.bfloat16)).astype(jnp.float32)


def reference(strain, basis_vectors, coefficients, template_rows):
    slice_len = SIDE // N_BASIS
    widened = basis_vectors.astype(jnp.float32)
    basis_re = widened[:, :, 0]
    basis_im = widened[:, :, 1]
    chosen = rounded(coefficients[template_rows])
    coeff_re = chosen[:, 0]
    coeff_im = chosen[:, 1]

    def owner_power(inputs):
        series_re, series_im = inputs
        flat_re = series_re.reshape(BASIS_VECS, slice_len * SIDE)
        flat_im = series_im.reshape(BASIS_VECS, slice_len * SIDE)
        rho_re = jnp.dot(coeff_re, flat_re, precision=highest) - jnp.dot(coeff_im, flat_im, precision=highest)
        rho_im = jnp.dot(coeff_re, flat_im, precision=highest) + jnp.dot(coeff_im, flat_re, precision=highest)
        return (rho_re * rho_re + rho_im * rho_im).reshape(TEMPLATES, slice_len, SIDE)

    def arrange(values):
        grid = values.reshape(BASIS_VECS, SIDE, SIDE)
        grid = jnp.transpose(grid, (0, 2, 1)).reshape(BASIS_VECS, N_BASIS, slice_len, SIDE)
        return jnp.transpose(grid, (1, 0, 2, 3))

    def one_segment(segment):
        strain_re = segment[:, 0]
        strain_im = segment[:, 1]
        prod_re = basis_re * strain_re + basis_im * strain_im
        prod_im = basis_re * strain_im - basis_im * strain_re
        spectrum = lax.complex(prod_re, prod_im)
        spectrum = jnp.transpose(spectrum, (0, 2, 1)).reshape(BASIS_VECS, SAMPLES // 2)
        spectrum = jnp.concatenate([spectrum, jnp.zeros_like(spectrum)], axis=1)
        series = jnp.fft.ifft(spectrum, axis=1) * SAMPLES
        grid_re = arrange(rounded(jnp.real(series)))
        grid_im = arrange(rounded(jnp.imag(series)))
        owners = lax.map(owner_power, (grid_re, grid_im))
        return jnp.transpose(owners, (1, 0, 2, 3)).reshape(TEMPLATES, SIDE, SIDE)

    return lax.map(one_segment, jnp.transpose(strain, (1, 0, 2, 3)))
```

```python
import functools
import math

import jax
import jax.numpy as jnp
import numpy as np
from jax import lax
from jax.experimental import pallas as pl
from jax.experimental.pallas import tpu as pltpu
from jax.sharding import PartitionSpec as P


highest = lax.Precision.HIGHEST
bf16 = jnp.bfloat16
f32 = jnp.float32


def rotation(left_index, right_index, period):
    turns = left_index * right_index % period
    angle = turns.astype(jnp.float32) * (2.0 * math.pi / period)
    return (jnp.cos(angle), jnp.sin(angle))


def complex_einsum(form, left_re, left_im, right_re, right_im):
    real_out = jnp.einsum(form, left_re, right_re, precision=highest) - jnp.einsum(
        form, left_im, right_im, precision=highest
    )
    imag_out = jnp.einsum(form, left_re, right_im, precision=highest) + jnp.einsum(
        form, left_im, right_re, precision=highest
    )
    return (real_out, imag_out)


def stack_rows(coeff_table, template_rows):
    chosen = coeff_table[template_rows].astype(jnp.bfloat16)
    return jnp.concatenate([chosen[:, 0], chosen[:, 1]], axis=0)


def rebuild(stacked, series_re, series_im):
    templates = stacked.shape[0] // 2
    left_sum = jnp.einsum("jk,sktu->sjtu", stacked, series_re, preferred_element_type=jnp.float32)
    right_sum = jnp.einsum("jk,sktu->sjtu", stacked, series_im, preferred_element_type=jnp.float32)
    rho_re = left_sum[:, :templates] - right_sum[:, templates:]
    rho_im = right_sum[:, :templates] + left_sum[:, templates:]
    return rho_re * rho_re + rho_im * rho_im


def general_shards(strain, basis_vectors, coefficients, template_rows):
    half_rows = strain.shape[3]
    side_len = 2 * half_rows
    samples = side_len * side_len
    freq_index = lax.broadcasted_iota(jnp.int32, (half_rows, side_len), 0)
    time_index = lax.broadcasted_iota(jnp.int32, (half_rows, side_len), 1)
    first_cos, first_sin = rotation(freq_index, time_index, side_len)
    column_index = lax.broadcasted_iota(jnp.int32, (side_len, side_len), 0)
    block_index = lax.broadcasted_iota(jnp.int32, (side_len, side_len), 1)
    second_cos, second_sin = rotation(column_index, block_index, side_len)
    coeff_table, whole_strain = (
        lax.all_gather(coefficients, "basis", axis=0, tiled=True),
        lax.all_gather(strain, "basis", axis=0, tiled=True),
    )
    stacked = stack_rows(coeff_table, template_rows)
    widened = basis_vectors.astype(jnp.float32)
    basis_re = widened[:, :, 0][None]
    basis_im = widened[:, :, 1][None]
    strain_re = jnp.transpose(whole_strain[:, :, 0], (1, 0, 2))[:, None]
    strain_im = jnp.transpose(whole_strain[:, :, 1], (1, 0, 2))[:, None]
    prod_re = basis_re * strain_re + basis_im * strain_im
    prod_im = basis_re * strain_im - basis_im * strain_re
    section_re, section_im = complex_einsum("skcr,rt->skct", prod_re, prod_im, first_cos, first_sin)
    twist_cos, twist_sin = rotation(column_index, block_index, samples)
    turned_re = section_re * twist_cos - section_im * twist_sin
    turned_im = section_re * twist_sin + section_im * twist_cos
    series_re, series_im = complex_einsum(
        "skct,cu->sktu", turned_re, turned_im, second_cos, second_sin
    )
    series_re = series_re.astype(jnp.bfloat16)
    series_im = series_im.astype(jnp.bfloat16)
    return rebuild(
        stacked,
        lax.all_to_all(series_re, "basis", split_axis=2, concat_axis=1, tiled=True),
        lax.all_to_all(series_im, "basis", split_axis=2, concat_axis=1, tiled=True),
    )


def split_const(x):
    hi = x.astype(bf16)
    return hi, (x - hi.astype(np.float32)).astype(bf16)


def unit_circle(turns, period):
    angle = (turns % period) * (2.0 * math.pi / period)
    return np.cos(angle).astype(np.float32), np.sin(angle).astype(np.float32)


def tables(side):
    own = side // 2
    r = np.arange(own)[None, :]
    first, twist = [], []
    for half in range(2):
        a = (half * own + np.arange(own))[:, None]
        cos, sin = unit_circle(a * r, side)
        first.append(np.block([[cos, -sin], [sin, cos]]))
        twist.append(np.stack(unit_circle(a * np.arange(side)[None, :], side * side)))
    hi, lo = split_const(np.stack(first))
    first = np.concatenate([hi, lo], axis=1)
    cos, sin = unit_circle(np.arange(side)[:, None] * np.arange(side)[None, :], side)
    second = np.stack(split_const(np.block([[cos, sin], [-sin, cos]])))
    return first, np.stack(twist), second


def dot(left, right):
    return jnp.dot(left, right, preferred_element_type=f32)


def dot_t(left, right):
    return lax.dot_general(left, right, (((1,), (1,)), ((), ())), preferred_element_type=f32)


def parts_of(x):
    hi = x.astype(bf16)
    return hi, (x - hi.astype(f32)).astype(bf16)


def series_kernel(half_ref, strain_ref, mine_ref, other_ref, first_ref, twist_ref, second_ref, out_ref, turned_ref):
    s = pl.program_id(0)
    half = half_ref[0]
    group, _, _, lanes = strain_ref.shape
    vecs, _, side, _ = mine_ref.shape
    cols = side // (2 * group)
    own = side // 2

    def segment(which):
        base = pl.multiple_of((s * 2 + which) * cols, cols)
        rows = [
            strain_ref[p, lax.bitwise_xor(half, q), pl.ds(base, cols), :]
            for q in range(2)
            for p in range(group)
        ]
        return jnp.concatenate(rows, axis=0).astype(f32)

    data_re, data_im = segment(0), segment(1)
    tiles = side // lanes
    for k in range(2 * vecs):
        ref = mine_ref if k < vecs else other_ref
        basis_re = ref[k % vecs, 0].astype(f32)
        basis_im = ref[k % vecs, 1].astype(f32)
        prod_re = basis_re * data_re + basis_im * data_im
        prod_im = basis_re * data_im - basis_im * data_re
        hi, lo = parts_of(jnp.concatenate([prod_re, prod_im], axis=1))
        both = dot_t(first_ref[0], hi)
        section = both[: 2 * own] + both[2 * own :] + dot_t(first_ref[0, : 2 * own], lo)
        section_re, section_im = section[:own], section[own:]
        turned_re = section_re * twist_ref[0, 0] - section_im * twist_ref[0, 1]
        turned_im = section_re * twist_ref[0, 1] + section_im * twist_ref[0, 0]
        for t in range(tiles):
            piece = slice(t * lanes, (t + 1) * lanes)
            turned_ref[t, pl.ds(k, own, stride=2 * vecs), :] = turned_re[:, piece]
            turned_ref[tiles + t, pl.ds(k, own, stride=2 * vecs), :] = turned_im[:, piece]
    hi, lo = parts_of(jnp.concatenate([turned_ref[t] for t in range(2 * tiles)], axis=1))
    series = dot(hi, second_ref[0]) + dot(lo, second_ref[0]) + dot(hi, second_ref[1])
    series = series.astype(bf16)
    block = out_ref.shape[3]
    for p in range(group):
        rows = series[p * block : (p + 1) * block]
        out_ref[p, 0, 0] = rows[:, :side]
        out_ref[p, 0, 1] = rows[:, side:]


def power_kernel(coeff_ref, series_ref, out_ref):
    group, _, _, rows, side = series_ref.shape
    chunks, height, _ = coeff_ref.shape
    sub = out_ref.shape[3] // 2
    step = rows // 2
    pairs = height // (2 * 2 * sub)
    right = [
        jnp.concatenate(
            [series_ref[p, 0, part, q * step : (q + 1) * step] for part in range(2) for p in range(group)],
            axis=0,
        )
        for q in range(2)
    ]
    low = lax.broadcasted_iota(jnp.int32, (pairs, 2 * sub, side), 1) < sub
    for chunk in range(chunks):
        left = coeff_ref[chunk]
        power = []
        for q in range(2):
            rho = dot(left, right[q])
            rho_re, rho_im = rho[: height // 2], rho[height // 2 :]
            power.append((rho_re * rho_re + rho_im * rho_im).reshape(pairs, 2 * sub, side))
        where = pl.ds(chunk * pairs, pairs)
        out_ref[0, where, 0] = jnp.where(low, power[0], pltpu.roll(power[1], sub, 1))
        out_ref[0, where, 1] = jnp.where(low, pltpu.roll(power[0], sub, 1), power[1])


def column_spread(group, vecs, quad):
    total = 2 * group * vecs
    spread = np.zeros((2, 2, 2 * total, 2, group, quad, 2, vecs), np.float32)
    for half, p, side, v in np.ndindex(2, group, 2, vecs):
        k = ((half ^ side) * group + p) * vecs + v
        spread[half, 0, k, 0, p, :, side, v] = 1.0
        spread[half, 0, total + k, 1, p, :, side, v] = -1.0
        spread[half, 1, total + k, 0, p, :, side, v] = 1.0
        spread[half, 1, k, 1, p, :, side, v] = 1.0
    return spread.reshape(2, 2, 2 * total, -1).astype(bf16)


def matrix_kernel(half_ref, place_ref, table_ref, spread_ref, out_ref, *, quad, block):
    chunks, height, width = out_ref.shape
    rows = table_ref.shape[0]
    span = height // 2
    own = lax.broadcasted_iota(jnp.int32, (span, width), 0) % quad
    col = lax.broadcasted_iota(jnp.int32, (span, width), 1) // block % quad
    for chunk in range(chunks):
        place = place_ref[:, chunk * span : (chunk + 1) * span]
        pick = lax.broadcasted_iota(jnp.int32, (rows, span), 0) == place
        pick = jnp.where(pick, 1.0, 0.0).astype(bf16)
        for part in range(2):
            wide = dot(table_ref[...], spread_ref[0, part]).astype(bf16)
            picked = lax.dot_general(pick, wide, (((0,), (0,)), ((), ())), preferred_element_type=f32)
            out_ref[chunk, part * span : (part + 1) * span] = jnp.where(own == col, picked, 0.0).astype(bf16)


def coefficient_matrix(table, template_rows, half, group, vecs, quad, chunks):
    per = table.shape[2]
    device, row = template_rows // per, template_rows % per
    place = ((device % group) * 2 + lax.bitwise_xor(device // group, half)) * per + row
    place = jnp.broadcast_to(place[:, None], (place.shape[0], quad)).reshape(1, -1)
    table = table.reshape(2 * group * per, -1)
    spread = column_spread(group, vecs, quad)
    shape = (chunks, 2 * place.shape[1] // chunks, spread.shape[3])
    return pl.pallas_call(
        functools.partial(matrix_kernel, quad=quad, block=2 * vecs),
        grid_spec=pltpu.PrefetchScalarGridSpec(
            num_scalar_prefetch=1,
            grid=(1,),
            in_specs=[
                pl.BlockSpec(place.shape, lambda i, h: (0, 0)),
                pl.BlockSpec(table.shape, lambda i, h: (0, 0)),
                pl.BlockSpec((1,) + spread.shape[1:], lambda i, h: (h[0], 0, 0, 0)),
            ],
            out_specs=pl.BlockSpec(shape, lambda i, h: (0, 0, 0)),
        ),
        out_shape=jax.ShapeDtypeStruct(shape, bf16),
        name="matrix",
    )(half[None], place, table, spread)


def halves_shards(n, strain, basis_vectors, coefficients, template_rows):
    cols, segs, _, lanes = strain.shape
    vecs, side = basis_vectors.shape[:2]
    group = n // 2
    own = side // 2
    per, _, total = coefficients.shape
    templates = template_rows.shape[0]
    quad = own // total
    chunks = 4
    across = [(i, i ^ group) for i in range(n)]
    halves = [list(range(group)), list(range(group, n))]
    half = lax.axis_index("basis") // group

    mine = jnp.transpose(basis_vectors, (0, 2, 1, 3))
    other = lax.ppermute(mine, "basis", across)
    narrow = jnp.transpose(strain, (1, 2, 0, 3)).reshape(segs * 2 * cols, lanes).astype(bf16)
    pack = jnp.concatenate([narrow, coefficients.astype(bf16).reshape(-1, lanes)], axis=0)
    pair = jnp.stack([pack, lax.ppermute(pack, "basis", across)])
    whole = lax.all_gather(pair, "basis", axis=0, axis_index_groups=halves)

    first, twist, second = tables(side)
    resident = lambda shape: pl.BlockSpec(shape, lambda s, h: (0,) * len(shape))
    by_half = lambda shape: pl.BlockSpec((1,) + shape[1:], lambda s, h: (h[0],) + (0,) * (len(shape) - 1))
    block = own // group * 2 * vecs
    series = pl.pallas_call(
        series_kernel,
        grid_spec=pltpu.PrefetchScalarGridSpec(
            num_scalar_prefetch=1,
            grid=(segs,),
            in_specs=[
                resident(whole.shape),
                resident(mine.shape),
                resident(mine.shape),
                by_half(first.shape),
                by_half(twist.shape),
                resident(second.shape),
            ],
            out_specs=pl.BlockSpec((group, 1, 2, block, side), lambda s, h: (0, s, 0, 0, 0)),
            scratch_shapes=[pltpu.VMEM((2 * side // lanes, own * 2 * vecs, lanes), f32)],
        ),
        out_shape=jax.ShapeDtypeStruct((group, segs, 2, block, side), bf16),
        name="series",
    )(half[None], whole, mine, other, first, twist, second)
    series = lax.all_to_all(series, "basis", split_axis=0, concat_axis=0, axis_index_groups=halves)

    table = whole[:, :, segs * 2 * cols :].reshape(group, 2, per, 2, total)
    matrix = coefficient_matrix(table, template_rows, half, group, vecs, quad, chunks)
    residues = own // group
    out = pl.pallas_call(
        power_kernel,
        grid=(segs, residues // (2 * quad)),
        in_specs=[
            pl.BlockSpec(matrix.shape, lambda s, g: (0, 0, 0)),
            pl.BlockSpec((group, 1, 2, 2 * quad * 2 * vecs, side), lambda s, g: (0, s, 0, g, 0)),
        ],
        out_specs=pl.BlockSpec((1, templates // 2, 2, 2 * quad, side), lambda s, g: (s, 0, 0, g, 0)),
        out_shape=jax.ShapeDtypeStruct((segs, templates // 2, 2, residues, side), f32),
        name="power",
    )(matrix, series)
    return out.reshape(segs, templates, residues, side)


def solution(mesh):
    in_specs = (
        P("basis", None, None, None),
        P(("bank", "basis"), None, None, None),
        P(("bank", "basis"), None, None),
        P("bank"),
    )
    out_specs = P(None, "bank", "basis", None)
    n = mesh.shape["basis"]

    def shards(strain, basis_vectors, coefficients, template_rows):
        lanes = strain.shape[3]
        total = coefficients.shape[2]
        quad = lanes // total
        fits = n % 2 == 0 and quad * 2 == 8 and basis_vectors.shape[1] % (16 * n) == 0
        plan = functools.partial(halves_shards, n) if fits else general_shards
        return plan(strain, basis_vectors, coefficients, template_rows)

    return jax.shard_map(shards, mesh=mesh, in_specs=in_specs, out_specs=out_specs, check_vma=False)
```

```python
import functools
import math

import jax
import jax.numpy as jnp
import numpy as np
from jax import lax
from jax.experimental import pallas as pl
from jax.experimental.pallas import tpu as pltpu
from jax.sharding import PartitionSpec as P


highest = lax.Precision.HIGHEST
bf16 = jnp.bfloat16
f32 = jnp.float32


def rotation(left_index, right_index, period):
    turns = left_index * right_index % period
    angle = turns.astype(jnp.float32) * (2.0 * math.pi / period)
    return (jnp.cos(angle), jnp.sin(angle))


def complex_einsum(form, left_re, left_im, right_re, right_im):
    real_out = jnp.einsum(form, left_re, right_re, precision=highest) - jnp.einsum(
        form, left_im, right_im, precision=highest
    )
    imag_out = jnp.einsum(form, left_re, right_im, precision=highest) + jnp.einsum(
        form, left_im, right_re, precision=highest
    )
    return (real_out, imag_out)


def stack_rows(coeff_table, template_rows):
    chosen = coeff_table[template_rows].astype(jnp.bfloat16)
    return jnp.concatenate([chosen[:, 0], chosen[:, 1]], axis=0)


def rebuild(stacked, series_re, series_im):
    templates = stacked.shape[0] // 2
    left_sum = jnp.einsum("jk,sktu->sjtu", stacked, series_re, preferred_element_type=jnp.float32)
    right_sum = jnp.einsum("jk,sktu->sjtu", stacked, series_im, preferred_element_type=jnp.float32)
    rho_re = left_sum[:, :templates] - right_sum[:, templates:]
    rho_im = right_sum[:, :templates] + left_sum[:, templates:]
    return rho_re * rho_re + rho_im * rho_im


def general_shards(strain, basis_vectors, coefficients, template_rows):
    half_rows = strain.shape[3]
    side_len = 2 * half_rows
    samples = side_len * side_len
    freq_index = lax.broadcasted_iota(jnp.int32, (half_rows, side_len), 0)
    time_index = lax.broadcasted_iota(jnp.int32, (half_rows, side_len), 1)
    first_cos, first_sin = rotation(freq_index, time_index, side_len)
    column_index = lax.broadcasted_iota(jnp.int32, (side_len, side_len), 0)
    block_index = lax.broadcasted_iota(jnp.int32, (side_len, side_len), 1)
    second_cos, second_sin = rotation(column_index, block_index, side_len)
    coeff_table, whole_strain = (
        lax.all_gather(coefficients, "basis", axis=0, tiled=True),
        lax.all_gather(strain, "basis", axis=0, tiled=True),
    )
    stacked = stack_rows(coeff_table, template_rows)
    widened = basis_vectors.astype(jnp.float32)
    basis_re = widened[:, :, 0][None]
    basis_im = widened[:, :, 1][None]
    strain_re = jnp.transpose(whole_strain[:, :, 0], (1, 0, 2))[:, None]
    strain_im = jnp.transpose(whole_strain[:, :, 1], (1, 0, 2))[:, None]
    prod_re = basis_re * strain_re + basis_im * strain_im
    prod_im = basis_re * strain_im - basis_im * strain_re
    section_re, section_im = complex_einsum("skcr,rt->skct", prod_re, prod_im, first_cos, first_sin)
    twist_cos, twist_sin = rotation(column_index, block_index, samples)
    turned_re = section_re * twist_cos - section_im * twist_sin
    turned_im = section_re * twist_sin + section_im * twist_cos
    series_re, series_im = complex_einsum(
        "skct,cu->sktu", turned_re, turned_im, second_cos, second_sin
    )
    series_re = series_re.astype(jnp.bfloat16)
    series_im = series_im.astype(jnp.bfloat16)
    return rebuild(
        stacked,
        lax.all_to_all(series_re, "basis", split_axis=2, concat_axis=1, tiled=True),
        lax.all_to_all(series_im, "basis", split_axis=2, concat_axis=1, tiled=True),
    )


def split_const(x):
    hi = x.astype(bf16)
    return hi, (x - hi.astype(np.float32)).astype(bf16)


def unit_circle(turns, period):
    angle = (turns % period) * (2.0 * math.pi / period)
    return np.cos(angle).astype(np.float32), np.sin(angle).astype(np.float32)


def tables(side):
    own = side // 2
    r = np.arange(own)[None, :]
    first, twist = [], []
    for half in range(2):
        a = (half * own + np.arange(own))[:, None]
        cos, sin = unit_circle(a * r, side)
        first.append(np.block([[cos, -sin], [sin, cos]]))
        twist.append(np.stack(unit_circle(a * np.arange(side)[None, :], side * side)))
    hi, lo = split_const(np.stack(first))
    first = np.concatenate([hi, lo], axis=1)
    cos, sin = unit_circle(np.arange(side)[:, None] * np.arange(side)[None, :], side)
    second = np.stack(split_const(np.block([[cos, sin], [-sin, cos]])))
    return first, np.stack(twist), second


def dot(left, right):
    return jnp.dot(left, right, preferred_element_type=f32)


def dot_t(left, right):
    return lax.dot_general(left, right, (((1,), (1,)), ((), ())), preferred_element_type=f32)


def parts_of(x):
    hi = x.astype(bf16)
    return hi, (x - hi.astype(f32)).astype(bf16)


def series_kernel(place_ref, *refs, group, start):
    packs, refs = refs[:group], refs[group:]
    mine_ref, other_ref, first_ref, twist_ref, second_ref, *outs, strain_ref, turned_ref, series_ref = refs
    half, spot = place_ref[0], place_ref[1]
    for m in range(group):
        strain_ref[lax.bitwise_xor(spot, m)] = packs[m][...]
    for s in range(outs[0].shape[0]):
        series_segment(
            half, start + s, strain_ref, mine_ref, other_ref, first_ref, twist_ref, second_ref, turned_ref, series_ref
        )
        for m in range(group):
            outs[m][s] = series_ref[lax.bitwise_xor(spot, m)]


def series_segment(
    half, s, strain_ref, mine_ref, other_ref, first_ref, twist_ref, second_ref, turned_ref, series_ref
):
    group, _, _, lanes = strain_ref.shape
    vecs, _, side, _ = mine_ref.shape
    cols = side // (2 * group)
    own = side // 2

    def segment(which):
        base = (s * 2 + which) * cols
        rows = [
            strain_ref[p, lax.bitwise_xor(half, q), base : base + cols]
            for q in range(2)
            for p in range(group)
        ]
        return jnp.concatenate(rows, axis=0).astype(f32)

    data_re, data_im = segment(0), segment(1)
    tiles = side // lanes
    for k in range(2 * vecs):
        ref = mine_ref if k < vecs else other_ref
        basis_re = ref[k % vecs, 0].astype(f32)
        basis_im = ref[k % vecs, 1].astype(f32)
        prod_re = basis_re * data_re + basis_im * data_im
        prod_im = basis_re * data_im - basis_im * data_re
        hi, lo = parts_of(jnp.concatenate([prod_re, prod_im], axis=1))
        both = dot_t(first_ref[half], hi)
        section = both[: 2 * own] + both[2 * own :] + dot_t(first_ref[half, : 2 * own], lo)
        section_re, section_im = section[:own], section[own:]
        turned_re = section_re * twist_ref[half, 0] - section_im * twist_ref[half, 1]
        turned_im = section_re * twist_ref[half, 1] + section_im * twist_ref[half, 0]
        for t in range(tiles):
            piece = slice(t * lanes, (t + 1) * lanes)
            turned_ref[t, pl.ds(k, own, stride=2 * vecs), :] = turned_re[:, piece]
            turned_ref[tiles + t, pl.ds(k, own, stride=2 * vecs), :] = turned_im[:, piece]
    hi, lo = parts_of(jnp.concatenate([turned_ref[t] for t in range(2 * tiles)], axis=1))
    series = dot(hi, second_ref[0]) + dot(lo, second_ref[0]) + dot(hi, second_ref[1])
    series = series.astype(bf16)
    block = series_ref.shape[2]
    for p in range(group):
        rows = series[p * block : (p + 1) * block]
        series_ref[p, 0] = rows[:, :side]
        series_ref[p, 1] = rows[:, side:]


def power_kernel(coeff_ref, *refs, group, start):
    series = refs[:group]
    out_ref, held_ref, sems = refs[-3:]
    segs, _, rows, side = series[0].shape
    chunks, height, _ = coeff_ref.shape
    residues = held_ref.shape[4]
    quad = 4
    quads = residues // quad
    step = rows // quads
    pairs = held_ref.shape[2]
    low = lax.broadcasted_iota(jnp.int32, (pairs, 2 * quad, side), 1) < quad
    copies = []
    for s in range(segs):
        right = [
            jnp.concatenate(
                [series[m][s, part, q * step : (q + 1) * step] for part in range(2) for m in range(group)],
                axis=0,
            )
            for q in range(quads)
        ]
        for chunk in range(chunks):
            for q in range(0, quads, 2):
                power = []
                for each in range(2):
                    rho = dot(coeff_ref[chunk], right[q + each])
                    rho_re, rho_im = rho[: height // 2], rho[height // 2 :]
                    power.append((rho_re * rho_re + rho_im * rho_im).reshape(pairs, 2 * quad, side))
                place = slice(q * quad, (q + 2) * quad)
                held_ref[s, chunk, :, 0, place] = jnp.where(low, power[0], pltpu.roll(power[1], quad, 1))
                held_ref[s, chunk, :, 1, place] = jnp.where(low, pltpu.roll(power[0], quad, 1), power[1])
            copy = pltpu.make_async_copy(
                held_ref.at[s, chunk],
                out_ref.at[start + s, pl.ds(chunk * pairs, pairs)],
                sems.at[s, chunk],
            )
            copy.start()
            copies.append(copy)
    for copy in copies:
        copy.wait()


def matrix_kernel(place_ref, rows_ref, *refs, quad, vecs, per):
    *packs, out_ref = refs
    group = len(packs)
    half, spot = place_ref[0], place_ref[1]
    chunks, height, width = out_ref.shape
    span = height // 2
    lanes = packs[0].shape[2]
    total = 2 * group * vecs
    iota = lambda shape, axis: lax.broadcasted_iota(jnp.int32, shape, axis)
    as_one = lambda test: jnp.where(test, 1.0, 0.0)

    table = jnp.concatenate(
        [packs[m][q, packs[m].shape[1] - per :] for m in range(group) for q in range(2)], axis=0
    )
    row, col = iota((lanes, width), 0), iota((lanes, width), 1)
    which = col // (width // 2)
    offset = col // (quad * 2 * vecs) % group
    source = lax.bitwise_xor(col // vecs % 2, half) * group + lax.bitwise_xor(offset, spot)
    index = source * vecs + col % vecs
    from_re = as_one(row == index)
    from_im = as_one(row == index + total)
    spread = [
        jnp.where(which == 0, from_re, -from_im).astype(bf16),
        jnp.where(which == 0, from_im, from_re).astype(bf16),
    ]
    device = rows_ref[...] // per
    place = lax.bitwise_xor(device % group, spot) * 2 + lax.bitwise_xor(device // group, half)
    place = place * per + rows_ref[...] % per
    pick = as_one(iota((table.shape[0], place.shape[1]), 0) == place).astype(bf16)
    chosen = lax.dot_general(pick, table, (((0,), (0,)), ((), ())), preferred_element_type=f32)
    chosen = chosen.astype(bf16)
    keep = iota((span, width), 0) % quad == iota((span, width), 1) // (2 * vecs) % quad
    wide = jnp.concatenate([dot(chosen, spread[part]).astype(bf16) for part in range(2)], axis=1)
    few = span // quad
    repeat = as_one(iota((span, few), 1) == iota((span, few), 0) // quad).astype(bf16)
    for chunk in range(chunks):
        block = dot(repeat, wide[chunk * few : (chunk + 1) * few])
        for part in range(2):
            half_block = block[:, part * width : (part + 1) * width]
            out_ref[chunk, part * span : (part + 1) * span] = jnp.where(keep, half_block, 0.0).astype(bf16)


def halves_shards(n, strain, basis_vectors, coefficients, template_rows):
    cols, segs, _, lanes = strain.shape
    vecs, side = basis_vectors.shape[:2]
    group = n // 2
    own = side // 2
    per, _, total = coefficients.shape
    templates = template_rows.shape[0]
    quad = own // total
    residues = own // group
    chunks = 4
    parts = 2
    spread = segs // parts
    to = lambda m: [(i, i ^ m) for i in range(n)]
    send = lambda x, m: lax.ppermute(x, "basis", to(m)) if m else x
    order = sorted(range(1, group), key=lambda m: -bin(m).count("1"))
    rank = lax.axis_index("basis")
    half, spot = rank // group, rank % group

    mine = jnp.transpose(basis_vectors, (0, 2, 1, 3))
    narrow = jnp.transpose(strain, (1, 2, 0, 3)).reshape(segs * 2 * cols, lanes).astype(bf16)
    coeff = coefficients.astype(bf16).reshape(per, 2 * total)
    coeff = jnp.pad(coeff, ((0, 0), (0, lanes - 2 * total)))
    pack = jnp.concatenate([narrow, coeff], axis=0)
    pair = jnp.stack([pack, send(pack, group)])
    other = send(mine, group)
    packs = [pair] * group
    for m in order:
        if m % 2 == 0:
            packs[m] = send(pair, m)
    for m in range(0, group, 2):
        packs[m + 1] = send(packs[m], 1)

    near = pl.BlockSpec(memory_space=pltpu.VMEM)
    far = pl.BlockSpec(memory_space=pl.ANY)
    scalars = pl.BlockSpec(memory_space=pltpu.SMEM)
    first, twist, second = tables(side)
    block = residues * 2 * vecs
    piece = (spread, 2, block, side)
    place = jnp.stack([half, spot])
    matrix_shape = (chunks, 2 * templates * quad // chunks, 2 * group * quad * 2 * vecs)
    received = []
    for part in range(parts):
        made = pl.pallas_call(
            functools.partial(series_kernel, group=group, start=part * spread),
            in_specs=[scalars] + [near] * (group + 5),
            out_specs=[near] * group,
            scratch_shapes=[
                pltpu.VMEM((group,) + pair.shape, bf16),
                pltpu.VMEM((2 * side // lanes, own * 2 * vecs, lanes), f32),
                pltpu.VMEM((group,) + piece[1:], bf16),
            ],
            out_shape=[jax.ShapeDtypeStruct(piece, bf16)] * group,
            name=f"series_{part}",
        )(place, *packs, mine, other, first, twist, second)
        got = list(made)
        for m in order:
            got[m] = send(made[m], m)
        received.append(got)
    matrix = pl.pallas_call(
        functools.partial(matrix_kernel, quad=quad, vecs=vecs, per=per),
        in_specs=[scalars] + [near] * (group + 1),
        out_specs=near,
        out_shape=jax.ShapeDtypeStruct(matrix_shape, bf16),
        name="matrix",
    )(place, template_rows.reshape(1, -1), *packs)

    out = None
    for part in range(parts):
        kept = [] if out is None else [out]
        out = pl.pallas_call(
            functools.partial(power_kernel, group=group, start=part * spread),
            in_specs=[near] * (group + 1) + [far] * len(kept),
            out_specs=far,
            scratch_shapes=[
                pltpu.VMEM((spread, chunks, templates // 2 // chunks, 2, residues, side), f32),
                pltpu.SemaphoreType.DMA((spread, chunks)),
            ],
            out_shape=jax.ShapeDtypeStruct((segs, templates // 2, 2, residues, side), f32),
            input_output_aliases={group + 1: 0} if kept else {},
            name=f"power_{part}",
        )(matrix, *received[part], *kept)
    return out.reshape(segs, templates, residues, side)


def solution(mesh):
    in_specs = (
        P("basis", None, None, None),
        P(("bank", "basis"), None, None, None),
        P(("bank", "basis"), None, None),
        P("bank"),
    )
    out_specs = P(None, "bank", "basis", None)
    n = mesh.shape["basis"]

    def shards(strain, basis_vectors, coefficients, template_rows):
        lanes = strain.shape[3]
        total = coefficients.shape[2]
        quad = lanes // total
        fits = n > 2 and n & (n - 1) == 0 and quad * 2 == 8 and basis_vectors.shape[1] % (16 * n) == 0
        plan = functools.partial(halves_shards, n) if fits else general_shards
        return plan(strain, basis_vectors, coefficients, template_rows)

    return jax.shard_map(shards, mesh=mesh, in_specs=in_specs, out_specs=out_specs, check_vma=False)
```

```python
import functools
import math

import jax
import jax.numpy as jnp
import numpy as np
from jax import lax
from jax.experimental import pallas as pl
from jax.experimental.pallas import tpu as pltpu
from jax.sharding import PartitionSpec as P


highest = lax.Precision.HIGHEST
bf16 = jnp.bfloat16
f32 = jnp.float32


def rotation(left_index, right_index, period):
    turns = left_index * right_index % period
    angle = turns.astype(jnp.float32) * (2.0 * math.pi / period)
    return (jnp.cos(angle), jnp.sin(angle))


def complex_einsum(form, left_re, left_im, right_re, right_im):
    real_out = jnp.einsum(form, left_re, right_re, precision=highest) - jnp.einsum(
        form, left_im, right_im, precision=highest
    )
    imag_out = jnp.einsum(form, left_re, right_im, precision=highest) + jnp.einsum(
        form, left_im, right_re, precision=highest
    )
    return (real_out, imag_out)


def stack_rows(coeff_table, template_rows):
    chosen = coeff_table[template_rows].astype(jnp.bfloat16)
    return jnp.concatenate([chosen[:, 0], chosen[:, 1]], axis=0)


def rebuild(stacked, series_re, series_im):
    templates = stacked.shape[0] // 2
    left_sum = jnp.einsum("jk,sktu->sjtu", stacked, series_re, preferred_element_type=jnp.float32)
    right_sum = jnp.einsum("jk,sktu->sjtu", stacked, series_im, preferred_element_type=jnp.float32)
    rho_re = left_sum[:, :templates] - right_sum[:, templates:]
    rho_im = right_sum[:, :templates] + left_sum[:, templates:]
    return rho_re * rho_re + rho_im * rho_im


def general_shards(strain, basis_vectors, coefficients, template_rows):
    half_rows = strain.shape[3]
    side_len = 2 * half_rows
    samples = side_len * side_len
    freq_index = lax.broadcasted_iota(jnp.int32, (half_rows, side_len), 0)
    time_index = lax.broadcasted_iota(jnp.int32, (half_rows, side_len), 1)
    first_cos, first_sin = rotation(freq_index, time_index, side_len)
    column_index = lax.broadcasted_iota(jnp.int32, (side_len, side_len), 0)
    block_index = lax.broadcasted_iota(jnp.int32, (side_len, side_len), 1)
    second_cos, second_sin = rotation(column_index, block_index, side_len)
    coeff_table, whole_strain = (
        lax.all_gather(coefficients, "basis", axis=0, tiled=True),
        lax.all_gather(strain, "basis", axis=0, tiled=True),
    )
    stacked = stack_rows(coeff_table, template_rows)
    widened = basis_vectors.astype(jnp.float32)
    basis_re = widened[:, :, 0][None]
    basis_im = widened[:, :, 1][None]
    strain_re = jnp.transpose(whole_strain[:, :, 0], (1, 0, 2))[:, None]
    strain_im = jnp.transpose(whole_strain[:, :, 1], (1, 0, 2))[:, None]
    prod_re = basis_re * strain_re + basis_im * strain_im
    prod_im = basis_re * strain_im - basis_im * strain_re
    section_re, section_im = complex_einsum("skcr,rt->skct", prod_re, prod_im, first_cos, first_sin)
    twist_cos, twist_sin = rotation(column_index, block_index, samples)
    turned_re = section_re * twist_cos - section_im * twist_sin
    turned_im = section_re * twist_sin + section_im * twist_cos
    series_re, series_im = complex_einsum(
        "skct,cu->sktu", turned_re, turned_im, second_cos, second_sin
    )
    series_re = series_re.astype(jnp.bfloat16)
    series_im = series_im.astype(jnp.bfloat16)
    return rebuild(
        stacked,
        lax.all_to_all(series_re, "basis", split_axis=2, concat_axis=1, tiled=True),
        lax.all_to_all(series_im, "basis", split_axis=2, concat_axis=1, tiled=True),
    )


def split_const(x):
    hi = x.astype(bf16)
    return hi, (x - hi.astype(np.float32)).astype(bf16)


def unit_circle(turns, period):
    angle = (turns % period) * (2.0 * math.pi / period)
    return np.cos(angle).astype(np.float32), np.sin(angle).astype(np.float32)


def tables(side):
    own = side // 2
    r = np.arange(own)[None, :]
    first, twist = [], []
    for half in range(2):
        a = (half * own + np.arange(own))[:, None]
        cos, sin = unit_circle(a * r, side)
        first.append(np.block([[cos, -sin], [sin, cos]]))
        twist.append(np.stack(unit_circle(a * np.arange(side)[None, :], side * side)))
    hi, lo = split_const(np.stack(first))
    first = np.concatenate([hi, lo], axis=1)
    cos, sin = unit_circle(np.arange(side)[:, None] * np.arange(side)[None, :], side)
    second = np.stack(split_const(np.block([[cos, sin], [-sin, cos]])))
    return first, np.stack(twist), second


def dot(left, right):
    return jnp.dot(left, right, preferred_element_type=f32)


def dot_t(left, right):
    return lax.dot_general(left, right, (((1,), (1,)), ((), ())), preferred_element_type=f32)


def parts_of(x):
    hi = x.astype(bf16)
    return hi, (x - hi.astype(f32)).astype(bf16)


def series_kernel(place_ref, *refs, group, start, slots):
    packs, refs = refs[:group], refs[group:]
    mine_ref, other_ref, first_ref, twist_ref, second_ref, *outs, strain_ref, turned_ref, series_ref = refs
    half, spot = place_ref[0], place_ref[1]
    for m in range(group):
        strain_ref[lax.bitwise_xor(spot, m)] = packs[m][...]
    for s in range(outs[0].shape[0]):
        series_segment(
            half, start + s, strain_ref, mine_ref, other_ref, first_ref, twist_ref, second_ref, turned_ref, series_ref
        )
        for out, m in zip(outs, slots):
            out[s] = series_ref[lax.bitwise_xor(spot, m)]


def tables_kernel(place_ref, pair_ref, first_ref, twist_ref, second_ref, *refs):
    *outs, copied_ref, sems = refs
    half = place_ref[0]
    copied_ref[...] = pair_ref[...]
    sources = first_ref.at[half], twist_ref.at[half], second_ref
    copies = [pltpu.make_async_copy(ref, out, sems.at[i]) for i, (ref, out) in enumerate(zip(sources, outs))]
    for copy in copies:
        copy.start()
    for copy in copies:
        copy.wait()


def series_segment(
    half, s, strain_ref, mine_ref, other_ref, first_ref, twist_ref, second_ref, turned_ref, series_ref
):
    group, _, _, lanes = strain_ref.shape
    vecs, _, side, _ = mine_ref.shape
    cols = side // (2 * group)
    own = side // 2

    def segment(which):
        base = (s * 2 + which) * cols
        rows = [
            strain_ref[p, lax.bitwise_xor(half, q), base : base + cols]
            for q in range(2)
            for p in range(group)
        ]
        return jnp.concatenate(rows, axis=0).astype(f32)

    data_re, data_im = segment(0), segment(1)
    tiles = side // lanes
    for k in range(2 * vecs):
        ref = mine_ref if k < vecs else other_ref
        basis_re = ref[k % vecs, 0].astype(f32)
        basis_im = ref[k % vecs, 1].astype(f32)
        prod_re = basis_re * data_re + basis_im * data_im
        prod_im = basis_re * data_im - basis_im * data_re
        hi, lo = parts_of(jnp.concatenate([prod_re, prod_im], axis=1))
        both = dot_t(first_ref[...], hi)
        section = both[: 2 * own] + both[2 * own :] + dot_t(first_ref[: 2 * own], lo)
        section_re, section_im = section[:own], section[own:]
        turned_re = section_re * twist_ref[0] - section_im * twist_ref[1]
        turned_im = section_re * twist_ref[1] + section_im * twist_ref[0]
        for t in range(tiles):
            piece = slice(t * lanes, (t + 1) * lanes)
            turned_ref[t, pl.ds(k, own, stride=2 * vecs), :] = turned_re[:, piece]
            turned_ref[tiles + t, pl.ds(k, own, stride=2 * vecs), :] = turned_im[:, piece]
    hi, lo = parts_of(jnp.concatenate([turned_ref[t] for t in range(2 * tiles)], axis=1))
    series = dot(hi, second_ref[0]) + dot(lo, second_ref[0]) + dot(hi, second_ref[1])
    series = series.astype(bf16)
    block = series_ref.shape[2]
    for p in range(group):
        rows = series[p * block : (p + 1) * block]
        series_ref[p, 0] = rows[:, :side]
        series_ref[p, 1] = rows[:, side:]


def power_kernel(coeff_ref, *refs, group, start, slots):
    series = [refs[slots.index(m)] for m in range(group)]
    out_ref, held_ref, sems = refs[-3:]
    segs, _, rows, side = series[0].shape
    chunks, height, _ = coeff_ref.shape
    residues = held_ref.shape[4]
    quad = 4
    quads = residues // quad
    step = rows // quads
    pairs = held_ref.shape[2]
    low = lax.broadcasted_iota(jnp.int32, (pairs, 2 * quad, side), 1) < quad
    copies = []
    for s in range(segs):
        right = [
            jnp.concatenate(
                [series[m][s, part, q * step : (q + 1) * step] for part in range(2) for m in range(group)],
                axis=0,
            )
            for q in range(quads)
        ]
        for chunk in range(chunks):
            for q in range(0, quads, 2):
                power = []
                for each in range(2):
                    rho = dot(coeff_ref[chunk], right[q + each])
                    rho_re, rho_im = rho[: height // 2], rho[height // 2 :]
                    power.append((rho_re * rho_re + rho_im * rho_im).reshape(pairs, 2 * quad, side))
                place = slice(q * quad, (q + 2) * quad)
                held_ref[s, chunk, :, 0, place] = jnp.where(low, power[0], pltpu.roll(power[1], quad, 1))
                held_ref[s, chunk, :, 1, place] = jnp.where(low, pltpu.roll(power[0], quad, 1), power[1])
            copy = pltpu.make_async_copy(
                held_ref.at[s, chunk],
                out_ref.at[start + s, pl.ds(chunk * pairs, pairs)],
                sems.at[s, chunk],
            )
            copy.start()
            copies.append(copy)
    for copy in copies:
        copy.wait()


def matrix_kernel(place_ref, rows_ref, *refs, quad, vecs, per):
    *packs, out_ref = refs
    group = len(packs)
    half, spot = place_ref[0], place_ref[1]
    chunks, height, width = out_ref.shape
    span = height // 2
    lanes = packs[0].shape[2]
    total = 2 * group * vecs
    iota = lambda shape, axis: lax.broadcasted_iota(jnp.int32, shape, axis)
    as_one = lambda test: jnp.where(test, 1.0, 0.0)

    table = jnp.concatenate(
        [packs[m][q, packs[m].shape[1] - per :] for m in range(group) for q in range(2)], axis=0
    )
    row, col = iota((lanes, width), 0), iota((lanes, width), 1)
    which = col // (width // 2)
    offset = col // (quad * 2 * vecs) % group
    source = lax.bitwise_xor(col // vecs % 2, half) * group + lax.bitwise_xor(offset, spot)
    index = source * vecs + col % vecs
    from_re = as_one(row == index)
    from_im = as_one(row == index + total)
    spread = [
        jnp.where(which == 0, from_re, -from_im).astype(bf16),
        jnp.where(which == 0, from_im, from_re).astype(bf16),
    ]
    device = rows_ref[...] // per
    place = lax.bitwise_xor(device % group, spot) * 2 + lax.bitwise_xor(device // group, half)
    place = place * per + rows_ref[...] % per
    pick = as_one(iota((table.shape[0], place.shape[1]), 0) == place).astype(bf16)
    chosen = lax.dot_general(pick, table, (((0,), (0,)), ((), ())), preferred_element_type=f32)
    chosen = chosen.astype(bf16)
    keep = iota((span, width), 0) % quad == iota((span, width), 1) // (2 * vecs) % quad
    wide = jnp.concatenate([dot(chosen, spread[part]).astype(bf16) for part in range(2)], axis=1)
    few = span // quad
    repeat = as_one(iota((span, few), 1) == iota((span, few), 0) // quad).astype(bf16)
    for chunk in range(chunks):
        block = dot(repeat, wide[chunk * few : (chunk + 1) * few])
        for part in range(2):
            half_block = block[:, part * width : (part + 1) * width]
            out_ref[chunk, part * span : (part + 1) * span] = jnp.where(keep, half_block, 0.0).astype(bf16)


def halves_shards(n, strain, basis_vectors, coefficients, template_rows):
    cols, segs, _, lanes = strain.shape
    vecs, side = basis_vectors.shape[:2]
    group = n // 2
    own = side // 2
    per, _, total = coefficients.shape
    templates = template_rows.shape[0]
    quad = own // total
    residues = own // group
    chunks = 4
    parts = 2
    spread = segs // parts
    to = lambda m: [(i, i ^ m) for i in range(n)]
    send = lambda x, m: lax.ppermute(x, "basis", to(m)) if m else x
    hold = lambda x: pltpu.with_memory_space_constraint(x, pltpu.VMEM)
    order = sorted(range(1, group), key=lambda m: -bin(m).count("1"))
    slots = order + [0]
    rank = lax.axis_index("basis")
    half, spot = rank // group, rank % group

    mine = jnp.transpose(basis_vectors, (0, 2, 1, 3))
    narrow = jnp.transpose(strain, (1, 2, 0, 3)).reshape(segs * 2 * cols, lanes).astype(bf16)
    coeff = coefficients.astype(bf16).reshape(per, 2 * total)
    coeff = jnp.pad(coeff, ((0, 0), (0, lanes - 2 * total)))
    pack = jnp.concatenate([narrow, coeff], axis=0)
    pair = jnp.stack([pack, send(pack, group)])
    other = send(mine, group)
    near = pl.BlockSpec(memory_space=pltpu.VMEM)
    room = pltpu.CompilerParams(vmem_limit_bytes=28 << 20)
    far = pl.BlockSpec(memory_space=pl.ANY)
    scalars = pl.BlockSpec(memory_space=pltpu.SMEM)
    block = residues * 2 * vecs
    piece = (spread, 2, block, side)
    place = jnp.stack([half, spot])
    matrix_shape = (chunks, 2 * templates * quad // chunks, 2 * group * quad * 2 * vecs)
    sources = tables(side)
    made = [pltpu.VMEM(x.shape[skip:], x.dtype) for x, skip in zip(sources, (1, 1, 0))]
    *rotations, copied = pl.pallas_call(
        tables_kernel,
        in_specs=[scalars, near] + [pl.BlockSpec(memory_space=pltpu.HBM)] * 3,
        out_specs=[near] * 4,
        out_shape=[*made, pltpu.VMEM(pair.shape, bf16)],
        scratch_shapes=[pltpu.SemaphoreType.DMA((3,))],
        compiler_params=room,
        name="tables",
    )(place, hold(pair), *sources)
    packs = [pair] * group
    for m in order:
        if m % 2 == 0:
            packs[m] = send(pair, m)
    for m in range(0, group, 2):
        packs[m + 1] = send(packs[m] if m else copied, 1)

    received = []
    for part in range(parts):
        made = pl.pallas_call(
            functools.partial(series_kernel, group=group, start=part * spread, slots=slots),
            in_specs=[scalars] + [near] * (group + 5),
            out_specs=[near] * group,
            scratch_shapes=[
                pltpu.VMEM((group,) + pair.shape, bf16),
                pltpu.VMEM((2 * side // lanes, own * 2 * vecs, lanes), f32),
                pltpu.VMEM((group,) + piece[1:], bf16),
            ],
            out_shape=[pltpu.VMEM(piece, bf16)] * group,
            compiler_params=room,
            name=f"series_{part}",
        )(place, *map(hold, packs), hold(mine), hold(other), *map(hold, rotations))
        received.append([send(x, m) for x, m in zip(made, slots)])
    matrix = pl.pallas_call(
        functools.partial(matrix_kernel, quad=quad, vecs=vecs, per=per),
        in_specs=[scalars] + [near] * (group + 1),
        out_specs=near,
        out_shape=pltpu.VMEM(matrix_shape, bf16),
        compiler_params=room,
        name="matrix",
    )(place, template_rows.reshape(1, -1), *map(hold, packs))

    out = None
    for part in range(parts):
        kept = [] if out is None else [out]
        out = pl.pallas_call(
            functools.partial(power_kernel, group=group, start=part * spread, slots=slots),
            in_specs=[near] * (group + 1) + [far] * len(kept),
            out_specs=far,
            scratch_shapes=[
                pltpu.VMEM((spread, chunks, templates // 2 // chunks, 2, residues, side), f32),
                pltpu.SemaphoreType.DMA((spread, chunks)),
            ],
            out_shape=jax.ShapeDtypeStruct((segs, templates // 2, 2, residues, side), f32),
            input_output_aliases={group + 1: 0} if kept else {},
            compiler_params=room,
            name=f"power_{part}",
        )(hold(matrix), *map(hold, received[part]), *kept)
    return out.reshape(segs, templates, residues, side)


def solution(mesh):
    in_specs = (
        P("basis", None, None, None),
        P(("bank", "basis"), None, None, None),
        P(("bank", "basis"), None, None),
        P("bank"),
    )
    out_specs = P(None, "bank", "basis", None)
    n = mesh.shape["basis"]

    def shards(strain, basis_vectors, coefficients, template_rows):
        lanes = strain.shape[3]
        total = coefficients.shape[2]
        quad = lanes // total
        fits = n > 2 and n & (n - 1) == 0 and quad * 2 == 8 and basis_vectors.shape[1] % (16 * n) == 0
        plan = functools.partial(halves_shards, n) if fits else general_shards
        return plan(strain, basis_vectors, coefficients, template_rows)

    return jax.shard_map(shards, mesh=mesh, in_specs=in_specs, out_specs=out_specs, check_vma=False)
```

```python
import functools
import math

import jax
import jax.numpy as jnp
import numpy as np
from jax import lax
from jax.experimental import pallas as pl
from jax.experimental.pallas import tpu as pltpu
from jax.sharding import PartitionSpec as P


highest = lax.Precision.HIGHEST
bf16 = jnp.bfloat16
f32 = jnp.float32


def rotation(left_index, right_index, period):
    turns = left_index * right_index % period
    angle = turns.astype(jnp.float32) * (2.0 * math.pi / period)
    return (jnp.cos(angle), jnp.sin(angle))


def complex_einsum(form, left_re, left_im, right_re, right_im):
    real_out = jnp.einsum(form, left_re, right_re, precision=highest) - jnp.einsum(
        form, left_im, right_im, precision=highest
    )
    imag_out = jnp.einsum(form, left_re, right_im, precision=highest) + jnp.einsum(
        form, left_im, right_re, precision=highest
    )
    return (real_out, imag_out)


def stack_rows(coeff_table, template_rows):
    chosen = coeff_table[template_rows].astype(jnp.bfloat16)
    return jnp.concatenate([chosen[:, 0], chosen[:, 1]], axis=0)


def rebuild(stacked, series_re, series_im):
    templates = stacked.shape[0] // 2
    left_sum = jnp.einsum("jk,sktu->sjtu", stacked, series_re, preferred_element_type=jnp.float32)
    right_sum = jnp.einsum("jk,sktu->sjtu", stacked, series_im, preferred_element_type=jnp.float32)
    rho_re = left_sum[:, :templates] - right_sum[:, templates:]
    rho_im = right_sum[:, :templates] + left_sum[:, templates:]
    return rho_re * rho_re + rho_im * rho_im


def general_shards(strain, basis_vectors, coefficients, template_rows):
    half_rows = strain.shape[3]
    side_len = 2 * half_rows
    samples = side_len * side_len
    freq_index = lax.broadcasted_iota(jnp.int32, (half_rows, side_len), 0)
    time_index = lax.broadcasted_iota(jnp.int32, (half_rows, side_len), 1)
    first_cos, first_sin = rotation(freq_index, time_index, side_len)
    column_index = lax.broadcasted_iota(jnp.int32, (side_len, side_len), 0)
    block_index = lax.broadcasted_iota(jnp.int32, (side_len, side_len), 1)
    second_cos, second_sin = rotation(column_index, block_index, side_len)
    coeff_table, whole_strain = (
        lax.all_gather(coefficients, "basis", axis=0, tiled=True),
        lax.all_gather(strain, "basis", axis=0, tiled=True),
    )
    stacked = stack_rows(coeff_table, template_rows)
    widened = basis_vectors.astype(jnp.float32)
    basis_re = widened[:, :, 0][None]
    basis_im = widened[:, :, 1][None]
    strain_re = jnp.transpose(whole_strain[:, :, 0], (1, 0, 2))[:, None]
    strain_im = jnp.transpose(whole_strain[:, :, 1], (1, 0, 2))[:, None]
    prod_re = basis_re * strain_re + basis_im * strain_im
    prod_im = basis_re * strain_im - basis_im * strain_re
    section_re, section_im = complex_einsum("skcr,rt->skct", prod_re, prod_im, first_cos, first_sin)
    twist_cos, twist_sin = rotation(column_index, block_index, samples)
    turned_re = section_re * twist_cos - section_im * twist_sin
    turned_im = section_re * twist_sin + section_im * twist_cos
    series_re, series_im = complex_einsum(
        "skct,cu->sktu", turned_re, turned_im, second_cos, second_sin
    )
    series_re = series_re.astype(jnp.bfloat16)
    series_im = series_im.astype(jnp.bfloat16)
    return rebuild(
        stacked,
        lax.all_to_all(series_re, "basis", split_axis=2, concat_axis=1, tiled=True),
        lax.all_to_all(series_im, "basis", split_axis=2, concat_axis=1, tiled=True),
    )


def split_const(x):
    hi = x.astype(bf16)
    return hi, (x - hi.astype(np.float32)).astype(bf16)


def unit_circle(turns, period):
    angle = (turns % period) * (2.0 * math.pi / period)
    return np.cos(angle).astype(np.float32), np.sin(angle).astype(np.float32)


def tables(side):
    own = side // 2
    r = np.arange(own)[None, :]
    first, twist = [], []
    for half in range(2):
        a = (half * own + np.arange(own))[:, None]
        cos, sin = unit_circle(a * r, side)
        first.append(np.block([[cos, -sin], [sin, cos]]))
        twist.append(np.stack(unit_circle(a * np.arange(side)[None, :], side * side)))
    hi, lo = split_const(np.stack(first))
    first = np.concatenate([hi, lo], axis=1)
    cos, sin = unit_circle(np.arange(side)[:, None] * np.arange(side)[None, :], side)
    second = np.stack(split_const(np.block([[cos, sin], [-sin, cos]])))
    return first, np.stack(twist), second


def dot(left, right):
    return jnp.dot(left, right, preferred_element_type=f32)


def dot_t(left, right):
    return lax.dot_general(left, right, (((1,), (1,)), ((), ())), preferred_element_type=f32)


def parts_of(x):
    hi = x.astype(bf16)
    return hi, (x - hi.astype(f32)).astype(bf16)


def series_kernel(place_ref, *refs, group, start, slots, quad, finish=None):
    packs, refs = refs[:group], refs[group:]
    basis_ref, first_ref, twist_ref, second_ref, *refs = refs
    if finish:
        rows_from, *refs, rows_ref, row_sem = refs
        *outs, matrix_ref, strain_ref, turned_ref, series_ref = refs
        fetch = pltpu.make_async_copy(rows_from, rows_ref, row_sem)
        fetch.start()
    else:
        *outs, strain_ref, turned_ref, series_ref = refs
    half, spot = place_ref[0], place_ref[1]
    for m in range(group):
        strain_ref[lax.bitwise_xor(spot, m)] = packs[m][...]
    batch = series_ref.shape[1]
    for s in range(0, outs[0].shape[0], batch):
        series_batch(
            half, start + s, quad, strain_ref, basis_ref, first_ref, twist_ref, second_ref, turned_ref, series_ref
        )
        for out, m in zip(outs, slots):
            out[s : s + batch] = series_ref[lax.bitwise_xor(spot, m)]
    if finish:
        fetch.wait()
        finish(place_ref, rows_ref, *packs, matrix_ref)


def tables_kernel(place_ref, pair_ref, first_ref, twist_ref, second_ref, *refs):
    *outs, copied_ref, sems = refs
    half = place_ref[0]
    copied_ref[...] = pair_ref[...]
    sources = first_ref.at[half], twist_ref.at[half], second_ref
    copies = [pltpu.make_async_copy(ref, out, sems.at[i]) for i, (ref, out) in enumerate(zip(sources, outs))]
    for copy in copies:
        copy.start()
    for copy in copies:
        copy.wait()


def series_batch(
    half, start, quad, strain_ref, basis_ref, first_ref, twist_ref, second_ref, turned_ref, series_ref
):
    group, _, _, lanes = strain_ref.shape
    vecs, _, side, _ = basis_ref.shape
    cols = side // (2 * group)
    own = side // 2
    tiles = side // lanes
    batch = series_ref.shape[1]

    def segment(s, which):
        base = (s * 2 + which) * cols
        rows = [
            strain_ref[p, lax.bitwise_xor(half, q), base : base + cols, :]
            for q in range(2)
            for p in range(group)
        ]
        return jnp.concatenate(rows, axis=0).astype(f32)

    for each in range(batch):
        data_re, data_im = segment(start + each, 0), segment(start + each, 1)
        for k in range(vecs):
            basis_re = basis_ref[k, 0].astype(f32)
            basis_im = basis_ref[k, 1].astype(f32)
            prod_re = basis_re * data_re + basis_im * data_im
            prod_im = basis_re * data_im - basis_im * data_re
            hi, lo = parts_of(jnp.concatenate([prod_re, prod_im], axis=1))
            both = dot_t(first_ref[...], hi)
            section = both[: 2 * own] + both[2 * own :] + dot_t(first_ref[: 2 * own], lo)
            section_re, section_im = section[:own], section[own:]
            turned_re = section_re * twist_ref[0] - section_im * twist_ref[1]
            turned_im = section_re * twist_ref[1] + section_im * twist_ref[0]
            where = pl.ds(each * own * vecs + k, own, stride=vecs)
            for t in range(tiles):
                piece = slice(t * lanes, (t + 1) * lanes)
                turned_ref[t, where, :] = turned_re[:, piece]
                turned_ref[tiles + t, where, :] = turned_im[:, piece]
    hi, lo = parts_of(jnp.concatenate([turned_ref[t] for t in range(2 * tiles)], axis=1))
    series = dot(hi, second_ref[0]) + dot(lo, second_ref[0]) + dot(hi, second_ref[1])
    step = quad * vecs
    series = [x.reshape(batch, own * vecs // step, step, side) for x in (series[:, :side], series[:, side:])]
    series = jnp.stack(series, axis=2).reshape(batch, group, -1, side).astype(bf16)
    for p in range(group):
        series_ref[p] = series[:, p]


def power_kernel(coeff_ref, *refs, group, start, slots, quad):
    early = [refs[slots[0].index(m)] for m in range(group)]
    late = [refs[group + slots[1].index(m)] for m in range(group)]
    out_ref, held_ref, sems = refs[-3:]
    segs, rows, side = late[0].shape
    chunks, height, _ = coeff_ref.shape
    residues = held_ref.shape[4]
    quads = residues // quad
    step = rows // quads
    pairs = held_ref.shape[2]
    low = lax.broadcasted_iota(jnp.int32, (pairs, 2 * quad, side), 1) < quad
    copies = []
    for s in range(segs):
        right = [
            jnp.concatenate(
                [x[start + s, q * step : (q + 1) * step] for x in early]
                + [x[s, q * step : (q + 1) * step] for x in late],
                axis=0,
            )
            for q in range(quads)
        ]
        for chunk in range(chunks):
            for q in range(0, quads, 2):
                power = []
                for each in range(2):
                    rho = dot(coeff_ref[chunk], right[q + each])
                    rho_re, rho_im = rho[: height // 2], rho[height // 2 :]
                    power.append((rho_re * rho_re + rho_im * rho_im).reshape(pairs, 2 * quad, side))
                place = slice(q * quad, (q + 2) * quad)
                held_ref[s, chunk, :, 0, place] = jnp.where(low, power[0], pltpu.roll(power[1], quad, 1))
                held_ref[s, chunk, :, 1, place] = jnp.where(low, pltpu.roll(power[0], quad, 1), power[1])
            copy = pltpu.make_async_copy(
                held_ref.at[s, chunk],
                out_ref.at[start + s, pl.ds(chunk * pairs, pairs)],
                sems.at[s, chunk],
            )
            copy.start()
            copies.append(copy)
    for copy in copies:
        copy.wait()


def matrix_kernel(place_ref, rows_ref, *refs, quad, vecs, per):
    *packs, out_ref = refs
    group = len(packs)
    half, spot = place_ref[0], place_ref[1]
    chunks, height, width = out_ref.shape
    span = height // 2
    lanes = packs[0].shape[2]
    total = 2 * group * vecs
    iota = lambda shape, axis: lax.broadcasted_iota(jnp.int32, shape, axis)
    as_one = lambda test: jnp.where(test, 1.0, 0.0)

    table = jnp.concatenate(
        [packs[m][q, packs[m].shape[1] - per :] for m in range(group) for q in range(2)], axis=0
    )
    row, col = iota((lanes, width), 0), iota((lanes, width), 1)
    which = col // (quad * vecs) % 2
    offset = col // (2 * quad * vecs) % group
    turn = col // (2 * quad * vecs * group)
    source = lax.bitwise_xor(turn, half) * group + lax.bitwise_xor(offset, spot)
    index = source * vecs + col % vecs
    from_re = as_one(row == index)
    from_im = as_one(row == index + total)
    spread = [
        jnp.where(which == 0, from_re, -from_im).astype(bf16),
        jnp.where(which == 0, from_im, from_re).astype(bf16),
    ]
    device = rows_ref[...] // per
    place = lax.bitwise_xor(device % group, spot) * 2 + lax.bitwise_xor(device // group, half)
    place = place * per + rows_ref[...] % per
    pick = as_one(iota((table.shape[0], place.shape[1]), 0) == place).astype(bf16)
    chosen = lax.dot_general(pick, table, (((0,), (0,)), ((), ())), preferred_element_type=f32)
    chosen = chosen.astype(bf16)
    keep = iota((span, width), 0) % quad == iota((span, width), 1) // vecs % quad
    wide = jnp.concatenate([dot(chosen, spread[part]).astype(bf16) for part in range(2)], axis=1)
    few = span // quad
    repeat = as_one(iota((span, few), 1) == iota((span, few), 0) // quad).astype(bf16)
    for chunk in range(chunks):
        block = dot(repeat, wide[chunk * few : (chunk + 1) * few])
        for part in range(2):
            half_block = block[:, part * width : (part + 1) * width]
            out_ref[chunk, part * span : (part + 1) * span] = jnp.where(keep, half_block, 0.0).astype(bf16)


def halves_shards(n, strain, basis_vectors, coefficients, template_rows):
    cols, segs, _, lanes = strain.shape
    vecs, side = basis_vectors.shape[:2]
    group = n // 2
    own = side // 2
    per, _, total = coefficients.shape
    templates = template_rows.shape[0]
    quad = own // total
    residues = own // group
    chunks = 4
    parts = 2
    spread = segs // parts
    to = lambda m: [(i, i ^ m) for i in range(n)]
    send = lambda x, m: lax.ppermute(x, "basis", to(m)) if m else x
    hold = lambda x: pltpu.with_memory_space_constraint(x, pltpu.VMEM)
    leave = lambda x: pltpu.with_memory_space_constraint(jnp.asarray(x), pltpu.HBM)
    rank = lax.axis_index("basis")
    half, spot = rank // group, rank % group

    mine = jnp.transpose(basis_vectors, (0, 2, 1, 3))
    narrow = jnp.transpose(strain, (1, 2, 0, 3)).reshape(segs * 2 * cols, lanes).astype(bf16)
    coeff = coefficients.astype(bf16).reshape(per, 2 * total)
    coeff = jnp.pad(coeff, ((0, 0), (0, lanes - 2 * total)))
    pack = jnp.concatenate([narrow, coeff], axis=0)
    pair = jnp.stack([pack, send(pack, group)])
    other = send(mine, group)
    near = pl.BlockSpec(memory_space=pltpu.VMEM)
    room = pltpu.CompilerParams(vmem_limit_bytes=28 << 20)
    far = pl.BlockSpec(memory_space=pl.ANY)
    scalars = pl.BlockSpec(memory_space=pltpu.SMEM)
    block = residues * 2 * vecs
    place = jnp.stack([half, spot])
    matrix_shape = (chunks, 2 * templates * quad // chunks, 2 * group * quad * 2 * vecs)
    sources = tables(side)
    made = [pltpu.VMEM(x.shape[skip:], x.dtype) for x, skip in zip(sources, (1, 1, 0))]
    *rotations, copied = pl.pallas_call(
        tables_kernel,
        in_specs=[scalars, near] + [pl.BlockSpec(memory_space=pltpu.HBM)] * 3,
        out_specs=[near] * 4,
        out_shape=[*made, pltpu.VMEM(pair.shape, bf16)],
        scratch_shapes=[pltpu.SemaphoreType.DMA((3,))],
        compiler_params=room,
        name="tables",
    )(place, hold(pair), *map(leave, sources))
    packs = [pair] * group
    for m in range(2, group, 2):
        packs[m] = send(pair, m)
    for m in range(0, group, 2):
        packs[m + 1] = send(packs[m] if m else copied, 1)


    finish = functools.partial(matrix_kernel, quad=quad, vecs=vecs, per=per)
    rows = template_rows.reshape(1, -1)
    matrices = []

    def exchange(basis, start, count, slots, last=False):
        piece = (count, block, side)
        made = [pltpu.VMEM(piece, bf16)] * group
        scratch = [
            pltpu.VMEM((group,) + pair.shape, bf16),
            pltpu.VMEM((2 * side // lanes, spread * own * vecs, lanes), f32),
            pltpu.VMEM((group, spread) + piece[1:], bf16),
        ]
        if last:
            made += [pltpu.VMEM(matrix_shape, bf16)]
            scratch += [pltpu.VMEM(rows.shape, jnp.int32), pltpu.SemaphoreType.DMA(())]
        made = pl.pallas_call(
            functools.partial(
                series_kernel, group=group, start=start, slots=slots, quad=quad, finish=finish if last else None
            ),
            in_specs=[scalars] + [near] * (group + 4) + [pl.BlockSpec(memory_space=pltpu.HBM)] * last,
            out_specs=[near] * len(made),
            scratch_shapes=scratch,
            out_shape=made,
            compiler_params=room,
        )(place, *map(hold, packs), hold(basis), *map(hold, rotations), *([leave(rows)] if last else []))
        matrices.extend(made[group:])
        return [send(x, m) for x, m in zip(made, slots)]

    far_first = lambda m: -bin(m).count("1")
    bases = sorted(range(2, group, 2), key=far_first)
    pairs = lambda bases: [m for base in bases for m in (base, base + 1)] + [1, 0]
    slots = pairs(sorted(bases, key=lambda m: m >= group // 2)), pairs(bases)
    early = exchange(mine, 0, segs, slots[0])
    late = [exchange(other, part * spread, spread, slots[1], part == parts - 1) for part in range(parts)]
    matrix = matrices[0]

    out = None
    for part in range(parts):
        kept = [] if out is None else [out]
        out = pl.pallas_call(
            functools.partial(power_kernel, group=group, start=part * spread, slots=slots, quad=quad),
            in_specs=[near] * (2 * group + 1) + [far] * len(kept),
            out_specs=far,
            scratch_shapes=[
                pltpu.VMEM((spread, chunks, templates // 2 // chunks, 2, residues, side), f32),
                pltpu.SemaphoreType.DMA((spread, chunks)),
            ],
            out_shape=jax.ShapeDtypeStruct((segs, templates // 2, 2, residues, side), f32),
            input_output_aliases={2 * group + 1: 0} if kept else {},
            compiler_params=room,
        )(hold(matrix), *map(hold, early), *map(hold, late[part]), *kept)
    return out.reshape(segs, templates, residues, side)


def solution(mesh):
    in_specs = (
        P("basis", None, None, None),
        P(("bank", "basis"), None, None, None),
        P(("bank", "basis"), None, None),
        P("bank"),
    )
    out_specs = P(None, "bank", "basis", None)
    n = mesh.shape["basis"]

    def shards(strain, basis_vectors, coefficients, template_rows):
        lanes = strain.shape[3]
        total = coefficients.shape[2]
        quad = lanes // total
        fits = n > 4 and n & (n - 1) == 0 and quad * 2 == 8 and quad * basis_vectors.shape[0] % 8 == 0 and basis_vectors.shape[1] % (16 * n) == 0
        plan = functools.partial(halves_shards, n) if fits else general_shards
        return plan(strain, basis_vectors, coefficients, template_rows)

    return jax.shard_map(shards, mesh=mesh, in_specs=in_specs, out_specs=out_specs, check_vma=False)
```

```python
import functools
import math

import jax
import jax.numpy as jnp
import numpy as np
from jax import lax
from jax.experimental import pallas as pl
from jax.experimental.pallas import tpu as pltpu
from jax.sharding import PartitionSpec as P


highest = lax.Precision.HIGHEST
bf16 = jnp.bfloat16
f32 = jnp.float32


def rotation(left_index, right_index, period):
    turns = left_index * right_index % period
    angle = turns.astype(jnp.float32) * (2.0 * math.pi / period)
    return (jnp.cos(angle), jnp.sin(angle))


def complex_einsum(form, left_re, left_im, right_re, right_im):
    real_out = jnp.einsum(form, left_re, right_re, precision=highest) - jnp.einsum(
        form, left_im, right_im, precision=highest
    )
    imag_out = jnp.einsum(form, left_re, right_im, precision=highest) + jnp.einsum(
        form, left_im, right_re, precision=highest
    )
    return (real_out, imag_out)


def stack_rows(coeff_table, template_rows):
    chosen = coeff_table[template_rows].astype(jnp.bfloat16)
    return jnp.concatenate([chosen[:, 0], chosen[:, 1]], axis=0)


def rebuild(stacked, series_re, series_im):
    templates = stacked.shape[0] // 2
    left_sum = jnp.einsum("jk,sktu->sjtu", stacked, series_re, preferred_element_type=jnp.float32)
    right_sum = jnp.einsum("jk,sktu->sjtu", stacked, series_im, preferred_element_type=jnp.float32)
    rho_re = left_sum[:, :templates] - right_sum[:, templates:]
    rho_im = right_sum[:, :templates] + left_sum[:, templates:]
    return rho_re * rho_re + rho_im * rho_im


def general_shards(strain, basis_vectors, coefficients, template_rows):
    half_rows = strain.shape[3]
    side_len = 2 * half_rows
    samples = side_len * side_len
    freq_index = lax.broadcasted_iota(jnp.int32, (half_rows, side_len), 0)
    time_index = lax.broadcasted_iota(jnp.int32, (half_rows, side_len), 1)
    first_cos, first_sin = rotation(freq_index, time_index, side_len)
    column_index = lax.broadcasted_iota(jnp.int32, (side_len, side_len), 0)
    block_index = lax.broadcasted_iota(jnp.int32, (side_len, side_len), 1)
    second_cos, second_sin = rotation(column_index, block_index, side_len)
    coeff_table, whole_strain = (
        lax.all_gather(coefficients, "basis", axis=0, tiled=True),
        lax.all_gather(strain, "basis", axis=0, tiled=True),
    )
    stacked = stack_rows(coeff_table, template_rows)
    widened = basis_vectors.astype(jnp.float32)
    basis_re = widened[:, :, 0][None]
    basis_im = widened[:, :, 1][None]
    strain_re = jnp.transpose(whole_strain[:, :, 0], (1, 0, 2))[:, None]
    strain_im = jnp.transpose(whole_strain[:, :, 1], (1, 0, 2))[:, None]
    prod_re = basis_re * strain_re + basis_im * strain_im
    prod_im = basis_re * strain_im - basis_im * strain_re
    section_re, section_im = complex_einsum("skcr,rt->skct", prod_re, prod_im, first_cos, first_sin)
    twist_cos, twist_sin = rotation(column_index, block_index, samples)
    turned_re = section_re * twist_cos - section_im * twist_sin
    turned_im = section_re * twist_sin + section_im * twist_cos
    series_re, series_im = complex_einsum(
        "skct,cu->sktu", turned_re, turned_im, second_cos, second_sin
    )
    series_re = series_re.astype(jnp.bfloat16)
    series_im = series_im.astype(jnp.bfloat16)
    return rebuild(
        stacked,
        lax.all_to_all(series_re, "basis", split_axis=2, concat_axis=1, tiled=True),
        lax.all_to_all(series_im, "basis", split_axis=2, concat_axis=1, tiled=True),
    )


def split_const(x):
    hi = x.astype(bf16)
    return hi, (x - hi.astype(np.float32)).astype(bf16)


def unit_circle(turns, period):
    angle = (turns % period) * (2.0 * math.pi / period)
    return np.cos(angle).astype(np.float32), np.sin(angle).astype(np.float32)


def tables(side):
    own = side // 2
    r = np.arange(own)[None, :]
    first, twist = [], []
    for half in range(2):
        a = (half * own + np.arange(own))[:, None]
        cos, sin = unit_circle(a * r, side)
        first.append(np.block([[cos, -sin], [sin, cos]]))
        twist.append(np.stack(unit_circle(a * np.arange(side)[None, :], side * side)))
    hi, lo = split_const(np.stack(first))
    first = np.concatenate([hi, lo], axis=1)
    cos, sin = unit_circle(np.arange(side)[:, None] * np.arange(side)[None, :], side)
    second = np.stack(split_const(np.block([[cos, sin], [-sin, cos]])))
    return first, np.stack(twist), second


def dot(left, right):
    return jnp.dot(left, right, preferred_element_type=f32)


def dot_t(left, right):
    return lax.dot_general(left, right, (((1,), (1,)), ((), ())), preferred_element_type=f32)


def parts_of(x):
    hi = x.astype(bf16)
    return hi, (x - hi.astype(f32)).astype(bf16)


def place_of(group):
    rank = lax.axis_index("basis")
    return lax.div(rank, group), lax.rem(rank, group)


def series_kernel(*refs, group, start, slots, quad, finish=None):
    packs, refs = refs[:group], refs[group:]
    basis_ref, first_ref, twist_ref, second_ref, *refs = refs
    if finish:
        rows_from, *refs, rows_ref, row_sem = refs
        *outs, matrix_ref, strain_ref, turned_ref, series_ref = refs
        fetch = pltpu.make_async_copy(rows_from, rows_ref, row_sem)
        fetch.start()
    else:
        *outs, strain_ref, turned_ref, series_ref = refs
    half, spot = place_of(group)
    for m in range(group):
        strain_ref[lax.bitwise_xor(spot, m)] = packs[m][...]
    batch = series_ref.shape[1]
    for s in range(0, outs[0].shape[0], batch):
        series_batch(
            half, start + s, quad, strain_ref, basis_ref, first_ref, twist_ref, second_ref, turned_ref, series_ref
        )
        for out, m in zip(outs, slots):
            out[s : s + batch] = series_ref[lax.bitwise_xor(spot, m)]
    if finish:
        fetch.wait()
        finish(half, spot, rows_ref, *packs, matrix_ref)


def tables_kernel(pair_ref, first_ref, twist_ref, second_ref, *refs, group):
    *outs, copied_ref, sems = refs
    half, _ = place_of(group)
    copied_ref[...] = pair_ref[...]
    sources = first_ref.at[half], twist_ref.at[half], second_ref
    copies = [pltpu.make_async_copy(ref, out, sems.at[i]) for i, (ref, out) in enumerate(zip(sources, outs))]
    for copy in copies:
        copy.start()
    for copy in copies:
        copy.wait()


def series_batch(
    half, start, quad, strain_ref, basis_ref, first_ref, twist_ref, second_ref, turned_ref, series_ref
):
    group, _, _, lanes = strain_ref.shape
    vecs, _, side, _ = basis_ref.shape
    cols = side // (2 * group)
    own = side // 2
    tiles = side // lanes
    batch = series_ref.shape[1]

    def segment(s, which):
        base = (s * 2 + which) * cols
        rows = [
            strain_ref[p, lax.bitwise_xor(half, q), base : base + cols, :]
            for q in range(2)
            for p in range(group)
        ]
        return jnp.concatenate(rows, axis=0).astype(f32)

    for each in range(batch):
        data_re, data_im = segment(start + each, 0), segment(start + each, 1)
        for k in range(vecs):
            basis_re = basis_ref[k, 0].astype(f32)
            basis_im = basis_ref[k, 1].astype(f32)
            prod_re = basis_re * data_re + basis_im * data_im
            prod_im = basis_re * data_im - basis_im * data_re
            hi, lo = parts_of(jnp.concatenate([prod_re, prod_im], axis=1))
            both = dot_t(first_ref[...], hi)
            section = both[: 2 * own] + both[2 * own :] + dot_t(first_ref[: 2 * own], lo)
            section_re, section_im = section[:own], section[own:]
            turned_re = section_re * twist_ref[0] - section_im * twist_ref[1]
            turned_im = section_re * twist_ref[1] + section_im * twist_ref[0]
            where = pl.ds(each * own * vecs + k, own, stride=vecs)
            for t in range(tiles):
                piece = slice(t * lanes, (t + 1) * lanes)
                turned_ref[t, where, :] = turned_re[:, piece]
                turned_ref[tiles + t, where, :] = turned_im[:, piece]
    hi, lo = parts_of(jnp.concatenate([turned_ref[t] for t in range(2 * tiles)], axis=1))
    series = dot(hi, second_ref[0]) + dot(lo, second_ref[0]) + dot(hi, second_ref[1])
    step = quad * vecs
    series = [x.reshape(batch, own * vecs // step, step, side) for x in (series[:, :side], series[:, side:])]
    series = jnp.stack(series, axis=2).reshape(batch, group, -1, side).astype(bf16)
    for p in range(group):
        series_ref[p] = series[:, p]


def power_kernel(coeff_ref, *refs, group, start, slots, quad):
    early = [refs[slots[0].index(m)] for m in range(group)]
    late = [refs[group + slots[1].index(m)] for m in range(group)]
    out_ref, held_ref, sems = refs[-3:]
    segs, rows, side = late[0].shape
    chunks, height, _ = coeff_ref.shape
    residues = held_ref.shape[4]
    quads = residues // quad
    step = rows // quads
    pairs = held_ref.shape[2]
    low = lax.broadcasted_iota(jnp.int32, (pairs, 2 * quad, side), 1) < quad
    copies = []
    for s in range(segs):
        right = [
            jnp.concatenate(
                [x[start + s, q * step : (q + 1) * step] for x in early]
                + [x[s, q * step : (q + 1) * step] for x in late],
                axis=0,
            )
            for q in range(quads)
        ]
        for chunk in range(chunks):
            for q in range(0, quads, 2):
                power = []
                for each in range(2):
                    rho = dot(coeff_ref[chunk], right[q + each])
                    rho_re, rho_im = rho[: height // 2], rho[height // 2 :]
                    power.append((rho_re * rho_re + rho_im * rho_im).reshape(pairs, 2 * quad, side))
                place = slice(q * quad, (q + 2) * quad)
                held_ref[s, chunk, :, 0, place] = jnp.where(low, power[0], pltpu.roll(power[1], quad, 1))
                held_ref[s, chunk, :, 1, place] = jnp.where(low, pltpu.roll(power[0], quad, 1), power[1])
            copy = pltpu.make_async_copy(
                held_ref.at[s, chunk],
                out_ref.at[start + s, pl.ds(chunk * pairs, pairs)],
                sems.at[s, chunk],
            )
            copy.start()
            copies.append(copy)
    for copy in copies:
        copy.wait()


def matrix_kernel(half, spot, rows_ref, *refs, quad, vecs, per):
    *packs, out_ref = refs
    group = len(packs)
    chunks, height, width = out_ref.shape
    span = height // 2
    lanes = packs[0].shape[2]
    total = 2 * group * vecs
    iota = lambda shape, axis: lax.broadcasted_iota(jnp.int32, shape, axis)
    as_one = lambda test: jnp.where(test, 1.0, 0.0)

    table = jnp.concatenate(
        [packs[m][q, packs[m].shape[1] - per :] for m in range(group) for q in range(2)], axis=0
    )
    row, col = iota((lanes, width), 0), iota((lanes, width), 1)
    which = col // (quad * vecs) % 2
    offset = col // (2 * quad * vecs) % group
    turn = col // (2 * quad * vecs * group)
    source = lax.bitwise_xor(turn, half) * group + lax.bitwise_xor(offset, spot)
    index = source * vecs + col % vecs
    from_re = as_one(row == index)
    from_im = as_one(row == index + total)
    spread = [
        jnp.where(which == 0, from_re, -from_im).astype(bf16),
        jnp.where(which == 0, from_im, from_re).astype(bf16),
    ]
    device = rows_ref[...] // per
    place = lax.bitwise_xor(device % group, spot) * 2 + lax.bitwise_xor(device // group, half)
    place = place * per + rows_ref[...] % per
    pick = as_one(iota((table.shape[0], place.shape[1]), 0) == place).astype(bf16)
    chosen = lax.dot_general(pick, table, (((0,), (0,)), ((), ())), preferred_element_type=f32)
    chosen = chosen.astype(bf16)
    keep = iota((span, width), 0) % quad == iota((span, width), 1) // vecs % quad
    wide = jnp.concatenate([dot(chosen, spread[part]).astype(bf16) for part in range(2)], axis=1)
    few = span // quad
    repeat = as_one(iota((span, few), 1) == iota((span, few), 0) // quad).astype(bf16)
    for chunk in range(chunks):
        block = dot(repeat, wide[chunk * few : (chunk + 1) * few])
        for part in range(2):
            half_block = block[:, part * width : (part + 1) * width]
            out_ref[chunk, part * span : (part + 1) * span] = jnp.where(keep, half_block, 0.0).astype(bf16)


def halves_shards(n, strain, basis_vectors, coefficients, template_rows):
    cols, segs, _, lanes = strain.shape
    vecs, side = basis_vectors.shape[:2]
    group = n // 2
    own = side // 2
    per, _, total = coefficients.shape
    templates = template_rows.shape[0]
    quad = own // total
    residues = own // group
    chunks = 8
    parts = 2
    spread = segs // parts
    to = lambda m: [(i, i ^ m) for i in range(n)]
    send = lambda x, m: lax.ppermute(x, "basis", to(m)) if m else x
    hold = lambda x: pltpu.with_memory_space_constraint(x, pltpu.VMEM)
    leave = lambda x: pltpu.with_memory_space_constraint(jnp.asarray(x), pltpu.HBM)

    mine = jnp.transpose(basis_vectors, (0, 2, 1, 3))
    narrow = jnp.transpose(strain, (1, 2, 0, 3)).reshape(segs * 2 * cols, lanes).astype(bf16)
    coeff = coefficients.astype(bf16).reshape(per, 2 * total)
    coeff = jnp.pad(coeff, ((0, 0), (0, lanes - 2 * total)))
    pack = jnp.concatenate([narrow, coeff], axis=0)
    pair = jnp.stack([pack, send(pack, group)])
    other = send(mine, group)
    near = pl.BlockSpec(memory_space=pltpu.VMEM)
    room = pltpu.CompilerParams(vmem_limit_bytes=28 << 20)
    far = pl.BlockSpec(memory_space=pl.ANY)
    block = residues * 2 * vecs
    matrix_shape = (chunks, 2 * templates * quad // chunks, 2 * group * quad * 2 * vecs)
    sources = tables(side)
    made = [pltpu.VMEM(x.shape[skip:], x.dtype) for x, skip in zip(sources, (1, 1, 0))]
    *rotations, copied = pl.pallas_call(
        functools.partial(tables_kernel, group=group),
        in_specs=[near] + [pl.BlockSpec(memory_space=pltpu.HBM)] * 3,
        out_specs=[near] * 4,
        out_shape=[*made, pltpu.VMEM(pair.shape, bf16)],
        scratch_shapes=[pltpu.SemaphoreType.DMA((3,))],
        compiler_params=room,
        name="tables",
    )(hold(pair), *map(leave, sources))
    packs = [pair] * group
    for m in range(2, group, 2):
        packs[m] = send(pair, m)
    for m in range(0, group, 2):
        packs[m + 1] = send(packs[m] if m else copied, 1)


    finish = functools.partial(matrix_kernel, quad=quad, vecs=vecs, per=per)
    rows = template_rows.reshape(1, -1)
    matrices = []

    def exchange(basis, start, count, slots, last=False):
        piece = (count, block, side)
        made = [pltpu.VMEM(piece, bf16)] * group
        scratch = [
            pltpu.VMEM((group,) + pair.shape, bf16),
            pltpu.VMEM((2 * side // lanes, spread * own * vecs, lanes), f32),
            pltpu.VMEM((group, spread) + piece[1:], bf16),
        ]
        if last:
            made += [pltpu.VMEM(matrix_shape, bf16)]
            scratch += [pltpu.VMEM(rows.shape, jnp.int32), pltpu.SemaphoreType.DMA(())]
        made = pl.pallas_call(
            functools.partial(
                series_kernel, group=group, start=start, slots=slots, quad=quad, finish=finish if last else None
            ),
            in_specs=[near] * (group + 4) + [pl.BlockSpec(memory_space=pltpu.HBM)] * last,
            out_specs=[near] * len(made),
            scratch_shapes=scratch,
            out_shape=made,
            compiler_params=room,
        )(*map(hold, packs), hold(basis), *map(hold, rotations), *([leave(rows)] if last else []))
        matrices.extend(made[group:])
        return [send(x, m) for x, m in zip(made, slots)]

    far_first = lambda m: -bin(m).count("1")
    bases = sorted(range(2, group, 2), key=far_first)
    pairs = lambda bases: [m for base in bases for m in (base, base + 1)] + [1, 0]
    slots = pairs(sorted(bases, key=lambda m: m >= group // 2)), pairs(bases)
    early = exchange(mine, 0, segs, slots[0])
    late = [exchange(other, part * spread, spread, slots[1], part == parts - 1) for part in range(parts)]
    matrix = matrices[0]

    out = None
    for part in range(parts):
        kept = [] if out is None else [out]
        out = pl.pallas_call(
            functools.partial(power_kernel, group=group, start=part * spread, slots=slots, quad=quad),
            in_specs=[near] * (2 * group + 1) + [far] * len(kept),
            out_specs=far,
            scratch_shapes=[
                pltpu.VMEM((spread, chunks, templates // 2 // chunks, 2, residues, side), f32),
                pltpu.SemaphoreType.DMA((spread, chunks)),
            ],
            out_shape=jax.ShapeDtypeStruct((segs, templates // 2, 2, residues, side), f32),
            input_output_aliases={2 * group + 1: 0} if kept else {},
            compiler_params=room,
        )(hold(matrix), *map(hold, early), *map(hold, late[part]), *kept)
    return out.reshape(segs, templates, residues, side)


def solution(mesh):
    in_specs = (
        P("basis", None, None, None),
        P(("bank", "basis"), None, None, None),
        P(("bank", "basis"), None, None),
        P("bank"),
    )
    out_specs = P(None, "bank", "basis", None)
    n = mesh.shape["basis"]

    def shards(strain, basis_vectors, coefficients, template_rows):
        lanes = strain.shape[3]
        total = coefficients.shape[2]
        quad = lanes // total
        fits = n > 4 and n & (n - 1) == 0 and quad * 2 == 8 and quad * basis_vectors.shape[0] % 8 == 0 and basis_vectors.shape[1] % (16 * n) == 0
        plan = functools.partial(halves_shards, n) if fits else general_shards
        return plan(strain, basis_vectors, coefficients, template_rows)

    return jax.shard_map(shards, mesh=mesh, in_specs=in_specs, out_specs=out_specs, check_vma=False)
```
